32 devices in a mesh: rep: 2 (over z, core), dp: 16 (over x, y).
Axes of the slice: x: 4, y: 4, z: 1, core: 2. Of those that a mesh axis runs over, the one named last changes fastest.
The devices are a block of a 4x4x8 slice.
Arguments:
- x: bfloat16 [32, 2048, 640], P(('rep', 'dp')), parts along dimension 0
- dy: bfloat16 [32, 2048, 640], P(('rep', 'dp')), parts along dimension 0
- w_gate: bfloat16 [2, 640, 2048], replicated
- w_up: bfloat16 [2, 640, 2048], replicated
- w_down: bfloat16 [2, 2048, 640], replicated
- m_w_gate: float32 [2, 640, 2048], P(None, 'dp')
- m_w_up: float32 [2, 640, 2048], P(None, 'dp')
- m_w_down: float32 [2, 2048, 640], P(None, 'dp')
- v_w_gate: float32 [2, 640, 2048], P(None, 'dp')
- v_w_up: float32 [2, 640, 2048], P(None, 'dp')
- v_w_down: float32 [2, 2048, 640], P(None, 'dp')
Outputs:
- output 1: bfloat16 [4, 640, 2048], P('rep'), parts along dimension 0
- output 2: bfloat16 [4, 640, 2048], P('rep'), parts along dimension 0
- output 3: bfloat16 [4, 2048, 640], P('rep'), parts along dimension 0
- output 4: float32 [4, 640, 2048], P('rep', 'dp'), parts along dimension 0
- output 5: float32 [4, 640, 2048], P('rep', 'dp'), parts along dimension 0
- output 6: float32 [4, 2048, 640], P('rep', 'dp'), parts along dimension 0
- output 7: float32 [4, 640, 2048], P('rep', 'dp'), parts along dimension 0
- output 8: float32 [4, 640, 2048], P('rep', 'dp'), parts along dimension 0
- output 9: float32 [4, 2048, 640], P('rep', 'dp'), parts along dimension 0
There are 2 independent parts. The reference program is written for one: setup_inputs(seed, part) draws one part's arguments, and reference() takes and returns one part's arrays. A program takes and returns all parts, laid end to end along the dimension named above; an argument that names none is the same for every part.
All inputs are finite; a program needn't handle non-finite values.
Results may differ from the reference program's by a relative error of at most 0.022.
Values are sent between devices in bfloat16 or wider.
A program may use at most 768 MiB of HBM per device.

```python
import jax
import jax.numpy as jnp
from jax import lax

SEQUENCES = 16
TOKENS = 2048
D = 640
FF = 2048
LAYERS = 2
NAMES = ("w_gate", "w_up", "w_down")
SHAPES = {"w_gate": (LAYERS, D, FF), "w_up": (LAYERS, D, FF), "w_down": (LAYERS, FF, D)}


def bump(key, n, height):
    away = (jnp.arange(n, dtype=jnp.int32) - jax.random.randint(key, (), 0, n, jnp.int32)) % n
    return jnp.where(away < n // 8, height, 1.0)


def together(key, own, strength):
    shared = jax.random.normal(key, own.shape[1:], jnp.float32)
    return (own + strength * shared) * lax.rsqrt(1 + strength * strength)


def setup_inputs(seed: int = 0, part: int = 0) -> dict:
    kx, kdy, ka, kb, kz, kf, kh, kl, *keys = jax.random.split(jax.random.key(seed), 8 + 3 * len(NAMES))
    kx, kdy, ka, kb = (jax.random.fold_in(k, part) for k in (kx, kdy, ka, kb))
    kw, km, kv = (keys[i::3] for i in range(3))
    shape = (SEQUENCES, TOKENS, D)
    much_x, much_dy = jax.random.uniform(kz, (2,), jnp.float32, 0.0, 1.0)
    loud = 2.0 ** jax.random.uniform(jax.random.fold_in(kz, 1), (), jnp.float32, -1.0, 2.0)
    layers = 2.0 ** jax.random.uniform(kl, (LAYERS, 1, 1), jnp.float32, -1.0, 1.0)
    x = together(ka, jax.random.normal(kx, shape, jnp.float32), much_x) * bump(kf, D, 4.0)
    dy = together(kb, jax.random.normal(kdy, shape, jnp.float32), much_dy)
    drawn = {"x": x.astype(jnp.bfloat16), "dy": (loud * dy * (SEQUENCES * TOKENS) ** -0.5).astype(jnp.bfloat16)}
    for key, name in zip(kw, NAMES, strict=True):
        w = jax.random.normal(key, SHAPES[name], jnp.float32) * SHAPES[name][1] ** -0.5
        drawn[name] = (w * {"w_gate": 1.0, "w_up": bump(kh, FF, 4.0), "w_down": layers}[name]).astype(jnp.bfloat16)
    for key, name in zip(km, NAMES, strict=True):
        drawn[f"m_{name}"] = 0.1 * jax.random.normal(key, SHAPES[name], jnp.float32)
    for key, name in zip(kv, NAMES, strict=True):
        drawn[f"v_{name}"] = jax.random.uniform(key, SHAPES[name], jnp.float32, 0.005, 0.015)
    return drawn


def matmul(a, w):
    return jnp.dot(a, w, preferred_element_type=jnp.float32).astype(jnp.bfloat16)


def normed(h):
    wide = h.astype(jnp.float32)
    scale = lax.rsqrt(jnp.mean(wide**2, -1, keepdims=True) + 1e-6)
    return (wide * scale).astype(jnp.bfloat16)


def layer(h, w):
    a = normed(h)
    gate = jnp.dot(a, w["w_gate"], preferred_element_type=jnp.float32)
    up = jnp.dot(a, w["w_up"], preferred_element_type=jnp.float32)
    return h + matmul((jax.nn.silu(gate) * up).astype(jnp.bfloat16), w["w_down"])


def adamw(w, m, v, g):
    m = 0.9 * m + 0.1 * g
    v = 0.95 * v + 0.05 * g * g
    step = m * lax.rsqrt(v + 1e-8) + 0.1 * w
    return (w - 0.02 * step).astype(jnp.bfloat16), m, v


def stack(weights, h):
    return lax.scan(lambda h, w: (layer(h, w), None), h, weights)[0]


def reference(x, dy, w_gate, w_up, w_down, m_w_gate, m_w_up, m_w_down, v_w_gate, v_w_up, v_w_down):
    weights = dict(zip(NAMES, (w_gate, w_up, w_down), strict=True))

    def take(so_far, sequence):
        h, by_y = sequence
        _, back = jax.vjp(lambda w: stack(w, h), weights)
        return jax.tree.map(lambda total, term: total + term.astype(jnp.float32), so_far, back(by_y)[0]), None

    none_yet = {name: jnp.zeros(w.shape, jnp.float32) for name, w in weights.items()}
    by_weights, _ = lax.scan(take, none_yet, (x, dy))
    gradients = [by_weights[name].astype(jnp.bfloat16).astype(jnp.float32) for name in NAMES]
    new = [
        adamw(w.astype(jnp.float32), m, v, g)
        for w, m, v, g in zip((w_gate, w_up, w_down), (m_w_gate, m_w_up, m_w_down), (v_w_gate, v_w_up, v_w_down), gradients, strict=True)
    ]
    return tuple(one[which] for which in range(3) for one in new)
```

```python
import functools
import math

import jax
import jax.numpy as jnp
from jax import lax
from jax.experimental import pallas as pl
from jax.experimental.pallas import tpu as pltpu
from jax.sharding import PartitionSpec as P

BF, F32 = jnp.bfloat16, jnp.float32
MESH = pl.DeviceIdType.MESH
ANY = pl.BlockSpec(memory_space=pl.ANY)
VMEM_LIMIT = 66 * 1024 * 1024 - 2 * 1024 * 1024

UNITS = (("d", 1), ("g", 1), ("u", 1), ("d", 0), ("g", 0), ("u", 0))
WIDE = (("g", 1), ("u", 1), ("g", 0), ("u", 0))
TALL = (("d", 1), ("d", 0))
LEFT_OF = {("d", 1): 0, ("g", 1): 1, ("u", 1): 1, ("d", 0): 2, ("g", 0): 3, ("u", 0): 3}
BLOCKS = 4


def adamw(w, m, v, g):
    m = 0.9 * m + 0.1 * g
    v = 0.95 * v + 0.05 * g * g
    step = m * lax.rsqrt(v + 1e-8) + 0.1 * w
    return (w - 0.02 * step).astype(BF), m, v


def step_kernel(side, rows, cols, *refs):
    lefts, rights = refs[0:4], refs[4:10]
    w_in, m_in, v_in = refs[10:13], refs[13:16], refs[16:19]
    w_out, m_out, v_out = refs[19:22], refs[22:25], refs[25:28]
    (gw, gt, r1w, r1t, r2w, r2t, left_buf, right_buf, ow, ot, mw, mt, vw, vt, g_full, send1, recv1, send2, recv2, left_sem, right_sem, state_sem, out_sem) = refs[28:]
    me = lax.axis_index("dp")
    at = (me // side, me % side)
    kinds = ("g", "u", "d")

    def index(x, y):
        return lax.rem(x + side, side) * side + lax.rem(y + side, side)

    def near(axis, by):
        return index(at[0] + by, at[1]) if axis == 0 else index(at[0], at[1] + by)

    def along(axis, by):
        return lax.rem(at[axis] + by + side, side)

    right_of, left_of = [near(a, 1) for a in (0, 1)], [near(a, -1) for a in (0, 1)]

    def part(unit, h, s):
        if unit[0] == "d":
            size = g_full.shape[0] // 4
            return (pl.ds((2 * h + s) * size, size), slice(None))
        size = gw.shape[-1] // 4
        return (slice(None), pl.ds((2 * h + s) * size, size))

    def pick(unit):
        if unit[0] == "d":
            n = TALL.index(unit)
            return gt.at[n], r1t.at[n], r2t.at[n]
        n = WIDE.index(unit)
        return gw.at[n], r1w.at[n], r2w.at[n]

    def several(unit, h, i, s):
        g = pick(unit)[0]
        lead = (i, slice(None)) if h == 0 else (slice(None), i)
        return g.at[lead + part(unit, h, s)]

    def single(unit, h, i, j, s):
        g = pick(unit)[0]
        lead = (i, j) if h == 0 else (j, i)
        return g.at[lead + part(unit, h, s)]

    def remote(src, dst, send, recv, to):
        return pltpu.make_async_remote_copy(src_ref=src, dst_ref=dst, send_sem=send, recv_sem=recv, device_id={"dp": to}, device_id_type=MESH)

    sent = []

    def push(src, dst, send, recv, to):
        copy = remote(src, dst, send, recv, to)
        copy.start()
        sent.append(copy)

    def arrived(dst, send, recv):
        remote(dst, dst, send, recv, right_of[0]).wait_recv()

    def phase1_send(unit):
        u = UNITS.index(unit)
        _, r1, _ = pick(unit)
        for h in (0, 1):
            far, nxt, prv = along(h, 2), along(h, 1), along(h, -1)
            for slot, src, to in ((0, several(unit, h, far, 1), right_of[h]), (1, several(unit, h, far, 0), left_of[h]), (2, several(unit, h, nxt, 0), right_of[h]), (3, several(unit, h, prv, 1), left_of[h])):
                push(src, r1.at[h, slot], send1.at[u, h, slot], recv1.at[u, h, slot], to)

    def phase1_pass(unit):
        u = UNITS.index(unit)
        _, r1, _ = pick(unit)
        for h in (0, 1):
            for slot, i, s, out, to in ((0, along(h, 1), 1, 4, right_of[h]), (1, along(h, -1), 0, 5, left_of[h])):
                arrived(r1.at[h, slot], send1.at[u, h, slot], recv1.at[u, h, slot])
                for j in range(side):
                    here = single(unit, h, i, j, s)
                    here[...] = (here[...].astype(F32) + r1[h, slot, j].astype(F32)).astype(BF)
                push(several(unit, h, i, s), r1.at[h, out], send1.at[u, h, out], recv1.at[u, h, out], to)

    def row_sum(unit, h, j, s):
        _, r1, _ = pick(unit)
        one, two = (2, 5) if s == 0 else (4, 3)
        return single(unit, h, at[h], j, s)[...].astype(F32) + r1[h, one, j].astype(F32) + r1[h, two, j].astype(F32)

    def phase2_send(unit):
        u = UNITS.index(unit)
        _, r1, r2 = pick(unit)
        for h in (0, 1):
            for slot in (2, 3, 4, 5):
                arrived(r1.at[h, slot], send1.at[u, h, slot], recv1.at[u, h, slot])
            o = 1 - h
            far, nxt, prv = along(o, 2), along(o, 1), along(o, -1)
            for slot, j, s, to in ((0, far, 1, right_of[o]), (1, far, 0, left_of[o]), (2, nxt, 0, right_of[o]), (3, prv, 1, left_of[o])):
                here = single(unit, h, at[h], j, s)
                here[...] = row_sum(unit, h, j, s).astype(BF)
                push(here, r2.at[h, slot], send1.at[u, h, 6 + slot], recv1.at[u, h, 6 + slot], to)

    def phase2_pass(unit):
        u = UNITS.index(unit)
        _, _, r2 = pick(unit)
        for h in (0, 1):
            o = 1 - h
            for slot, j, s, out, to in ((0, along(o, 1), 1, 4, right_of[o]), (1, along(o, -1), 0, 5, left_of[o])):
                arrived(r2.at[h, slot], send1.at[u, h, 6 + slot], recv1.at[u, h, 6 + slot])
                here = single(unit, h, at[h], j, s)
                here[...] = (row_sum(unit, h, j, s) + r2[h, slot].astype(F32)).astype(BF)
                push(here, r2.at[h, out], send1.at[u, h, 6 + out], recv1.at[u, h, 6 + out], to)

    def state(unit):
        k = kinds.index(unit[0])
        n = TALL.index(unit) if unit[0] == "d" else WIDE.index(unit)
        own, m, v = (ot, mt, vt) if unit[0] == "d" else (ow, mw, vw)
        return k, own.at[n], m.at[n], v.at[n]

    def state_copies(unit, which=(0, 1, 2)):
        u = UNITS.index(unit)
        k, own, m, v = state(unit)
        layer = unit[1]
        pairs = ((w_in[k].at[layer, me], own), (m_in[k].at[layer], m), (v_in[k].at[layer], v))
        return [pltpu.make_async_copy(*pairs[i], state_sem.at[u, i]) for i in which]

    def result_copies(unit, which=(0, 1, 2)):
        u = UNITS.index(unit)
        k, own, m, v = state(unit)
        layer = unit[1]
        pairs = ((own, w_out[k].at[layer, at[0], at[1]]), (m, m_out[k].at[layer]), (v, v_out[k].at[layer]))
        return [pltpu.make_async_copy(*pairs[i], out_sem.at[u, i]) for i in which]

    def total(unit, h, s):
        _, _, r2 = pick(unit)
        one, two = (2, 5) if s == 0 else (4, 3)
        g = row_sum(unit, h, at[1 - h], s) + r2[h, one].astype(F32) + r2[h, two].astype(F32)
        return g.astype(BF).astype(F32)

    def w_part(unit, h, s):
        k, own, _, _ = state(unit)
        if unit[0] == "d":
            size = own.shape[0] // 4
            start, count = ((2 * h + s) * size, size) if s is not None else (2 * h * size, 2 * size)
            return (pl.ds(start, count), slice(None))
        size = own.shape[1] // 4
        start, count = ((2 * h + s) * size, size) if s is not None else (2 * h * size, 2 * size)
        return (slice(None), pl.ds(start, count))

    def w_single(unit, h, i, j, s):
        k = kinds.index(unit[0])
        lead = (i, j) if h == 0 else (j, i)
        return w_out[k].at[(unit[1],) + lead + w_part(unit, h, s)]

    def w_several(unit, h, i, s):
        k = kinds.index(unit[0])
        lead = (i, slice(None)) if h == 0 else (slice(None), i)
        return w_out[k].at[(unit[1],) + lead + w_part(unit, h, s)]

    def update(unit):
        u = UNITS.index(unit)
        k, own, m, v = state(unit)
        for copy in state_copies(unit):
            copy.wait()
        for h in (0, 1):
            for slot in (2, 3, 4, 5):
                arrived(pick(unit)[2].at[h, slot], send1.at[u, h, 6 + slot], recv1.at[u, h, 6 + slot])
        if unit[0] == "d":
            for h in (0, 1):
                for s in (0, 1):
                    g_full[part(unit, h, s)[0], :] = total(unit, h, s)
            own[...], m[...], v[...] = adamw(own[...].astype(F32), m[...], v[...], g_full[...].T)
        else:
            for h in (0, 1):
                for s in (0, 1):
                    c = part(unit, h, s)
                    own[c], m[c], v[c] = adamw(own[c].astype(F32), m[c], v[c], total(unit, h, s))
        for copy in result_copies(unit):
            copy.start()
        for h in (0, 1):
            o = 1 - h
            src, dst = own.at[w_part(unit, h, None)], w_single(unit, h, at[h], at[o], None)
            push(src, dst, send2.at[u, h, 0], recv2.at[u, h, 0], right_of[o])
            push(src, dst, send2.at[u, h, 1], recv2.at[u, h, 1], left_of[o])

    def gather1_pass(unit):
        u = UNITS.index(unit)
        for h in (0, 1):
            o = 1 - h
            for slot, by, s, to in ((0, -1, 1, right_of[o]), (1, 1, 0, left_of[o])):
                arrived(w_single(unit, h, at[h], along(o, by), None), send2.at[u, h, slot], recv2.at[u, h, slot])
                piece = w_single(unit, h, at[h], along(o, by), s)
                push(piece, piece, send2.at[u, h, 2 + slot], recv2.at[u, h, 2 + slot], to)

    def gather2_send(unit):
        u = UNITS.index(unit)
        result_copies(unit, (0,))[0].wait()
        for h in (0, 1):
            o = 1 - h
            for slot, s in ((2, 1), (3, 0)):
                arrived(w_single(unit, h, at[h], along(o, 2), s), send2.at[u, h, slot], recv2.at[u, h, slot])
            piece = w_several(unit, h, at[h], None)
            push(piece, piece, send2.at[u, h, 4], recv2.at[u, h, 4], right_of[h])
            push(piece, piece, send2.at[u, h, 5], recv2.at[u, h, 5], left_of[h])

    def gather2_pass(unit):
        u = UNITS.index(unit)
        for h in (0, 1):
            for slot, by, s, to in ((4, -1, 1, right_of[h]), (5, 1, 0, left_of[h])):
                arrived(w_several(unit, h, along(h, by), None), send2.at[u, h, slot], recv2.at[u, h, slot])
                piece = w_several(unit, h, along(h, by), s)
                push(piece, piece, send2.at[u, h, 2 + slot], recv2.at[u, h, 2 + slot], to)

    def gather2_end(unit):
        u = UNITS.index(unit)
        for h in (0, 1):
            for slot, s in ((6, 1), (7, 0)):
                arrived(w_several(unit, h, along(h, 2), s), send2.at[u, h, slot], recv2.at[u, h, slot])

    width = right_buf.shape[-1]

    def left_copy(n):
        return pltpu.make_async_copy(lefts[n], left_buf.at[n % 2], left_sem.at[n % 2])

    def right_copy(u, n, slot):
        return pltpu.make_async_copy(rights[u].at[:, pl.ds(pl.multiple_of(n * width, width), width)], right_buf.at[slot], right_sem.at[slot])

    def gradient(unit):
        u = UNITS.index(unit)
        left = LEFT_OF[unit]
        if u == 0 or LEFT_OF[UNITS[u - 1]] != left:
            left_copy(left).wait()

        def block(n, _):
            slot = lax.rem(n, 2)

            @pl.when(n < BLOCKS - 1)
            def _():
                right_copy(u, n + 1, 1 - slot).start()

            if u + 1 < len(UNITS):

                @pl.when(n == BLOCKS - 1)
                def _():
                    right_copy(u + 1, 0, 1 - slot).start()

            right_copy(u, n, slot).wait()
            out = jnp.dot(left_buf[left % 2], right_buf[slot], preferred_element_type=F32)
            g = pick(unit)[0]
            if unit[0] == "d":
                for c in range(width // cols):
                    chunk = n * (width // cols) + c
                    g[chunk // side, lax.rem(chunk, side)] = out[:, c * cols : (c + 1) * cols].astype(BF)
            else:
                for x in range(side):
                    for y in range(side):
                        r = (x * side + y) * rows
                        g[x, y, :, pl.ds(pl.multiple_of(n * width, width), width)] = out[r : r + rows].astype(BF)
            return 0

        lax.fori_loop(0, BLOCKS, block, 0)
        if (u + 1 == len(UNITS) or LEFT_OF[UNITS[u + 1]] != left) and left + 2 < len(lefts):
            left_copy(left + 2).start()

    left_copy(0).start()
    right_copy(0, 0, 0).start()
    left_copy(1).start()
    for unit in UNITS:
        for copy in state_copies(unit):
            copy.start()
    barrier = pltpu.get_barrier_semaphore()
    for a in (0, 1):
        for to in (left_of[a], right_of[a]):
            pl.semaphore_signal(barrier, inc=1, device_id={"dp": to}, device_id_type=MESH)
    pl.semaphore_wait(barrier, 4)

    stages = (phase1_send, phase1_pass, phase2_send, phase2_pass, update, gather1_pass, gather2_send, gather2_pass, gather2_end)
    for t in range(len(UNITS) + len(stages) - 1):
        if t < len(UNITS):
            gradient(UNITS[t])
        for s, stage in enumerate(stages):
            if 0 <= t - s < len(UNITS):
                stage(UNITS[t - s])
    for unit in UNITS:
        for copy in result_copies(unit, (1, 2)):
            copy.wait()
    for copy in sent:
        copy.wait_send()


def reduce_step_gather(n, lefts, rights, weights, m, v):
    side = math.isqrt(n)
    layers, rows, ff = m[0].shape
    cols, d = m[2].shape[1:]
    blocked = [w.reshape(layers, n, -1, w.shape[-1]) for w in weights]
    half, part = ff // 2, ff // 4
    width = ff // BLOCKS
    out_shape = (
        [jax.ShapeDtypeStruct((layers, side, side, rows, ff), BF)] * 2
        + [jax.ShapeDtypeStruct((layers, side, side, cols, d), BF)]
        + [jax.ShapeDtypeStruct(t.shape, F32) for t in (*m, *v)]
    )
    nw, nt, nu = len(WIDE), len(TALL), len(UNITS)
    out = pl.pallas_call(
        functools.partial(step_kernel, side, rows, cols),
        out_shape=out_shape,
        in_specs=[ANY] * 19,
        out_specs=[ANY] * 9,
        scratch_shapes=[
            pltpu.VMEM((nw, side, side, rows, ff), BF),
            pltpu.VMEM((nt, side, side, d, cols), BF),
            pltpu.VMEM((nw, 2, 6, side, rows, part), BF),
            pltpu.VMEM((nt, 2, 6, side, d // 4, cols), BF),
            pltpu.VMEM((nw, 2, 6, rows, part), BF),
            pltpu.VMEM((nt, 2, 6, d // 4, cols), BF),
            pltpu.VMEM((2, d, lefts[0].shape[1]), BF),
            pltpu.VMEM((2, rights[0].shape[0], width), BF),
            pltpu.VMEM((nw, rows, ff), BF),
            pltpu.VMEM((nt, cols, d), BF),
            pltpu.VMEM((nw, rows, ff), F32),
            pltpu.VMEM((nt, cols, d), F32),
            pltpu.VMEM((nw, rows, ff), F32),
            pltpu.VMEM((nt, cols, d), F32),
            pltpu.VMEM((d, cols), F32),
            pltpu.SemaphoreType.DMA((nu, 2, 12)),
            pltpu.SemaphoreType.DMA((nu, 2, 12)),
            pltpu.SemaphoreType.DMA((nu, 2, 8)),
            pltpu.SemaphoreType.DMA((nu, 2, 8)),
            pltpu.SemaphoreType.DMA((2,)),
            pltpu.SemaphoreType.DMA((2,)),
            pltpu.SemaphoreType.DMA((nu, 3)),
            pltpu.SemaphoreType.DMA((nu, 3)),
        ],
        compiler_params=pltpu.CompilerParams(collective_id=0, has_side_effects=True, vmem_limit_bytes=VMEM_LIMIT),
        name="reduce_step_gather",
    )(*lefts, *rights, *blocked, *m, *v)
    return tuple(w.reshape(layers, -1, w.shape[-1]) for w in out[:3]) + tuple(out[3:])


def matmul(a, w):
    return jnp.dot(a, w, preferred_element_type=F32).astype(BF)


def matmul_t(a, w):
    return lax.dot_general(a, w, (((1,), (1,)), ((), ())), preferred_element_type=F32).astype(BF)


def normed(h):
    wide = h.astype(F32)
    scale = lax.rsqrt(jnp.mean(wide**2, -1, keepdims=True) + 1e-6)
    return (wide * scale).astype(BF), scale


def normed_back(h, scale, da):
    wide, da = h.astype(F32), da.astype(F32)
    inner = jnp.sum(da * wide, -1, keepdims=True)
    return (da * scale - wide * (scale * scale * scale * inner / h.shape[-1])).astype(BF)


def gated(gate, up):
    return (jax.nn.silu(gate) * up).astype(BF)


def gated_back(gate, up, d):
    sig = jax.nn.sigmoid(gate)
    silu = gate * sig
    d = d.astype(F32)
    return (d * up * (sig + silu * (1 - sig))).astype(BF), (d * silu).astype(BF)


def forward_backward(x, dy, w_gate, w_up, w_down):
    wide = functools.partial(jnp.dot, preferred_element_type=F32)
    a0, _ = normed(x)
    gate0, up0 = wide(a0, w_gate[0]), wide(a0, w_up[0])
    act0 = gated(gate0, up0)
    h = x + matmul(act0, w_down[0])
    a1, scale = normed(h)
    gate1, up1 = wide(a1, w_gate[1]), wide(a1, w_up[1])
    act1 = gated(gate1, up1)
    dg1, du1 = gated_back(gate1, up1, matmul_t(dy, w_down[1]))
    da = matmul_t(dg1, w_gate[1]) + matmul_t(du1, w_up[1])
    dh = dy + normed_back(h, scale, da)
    dg0, du0 = gated_back(gate0, up0, matmul_t(dh, w_down[0]))
    return (dy.T, a1.T, dh.T, a0.T), (act1, dg1, du1, act0, dg0, du0)


def solution(mesh):
    n = mesh.shape["dp"]

    def step(x, dy, *arrays):
        weights, m, v = (arrays[i : i + 3] for i in (0, 3, 6))
        lefts, rights = forward_backward(x[0], dy[0], *weights)
        return reduce_step_gather(n, lefts, rights, weights, m, v)

    rows = P(None, "dp", None)
    return jax.shard_map(
        step,
        mesh=mesh,
        in_specs=(P(("rep", "dp"), None, None),) * 2 + (P(None, None, None),) * 3 + (rows,) * 6,
        out_specs=(P("rep", None, None),) * 3 + (P("rep", "dp", None),) * 6,
        check_vma=False,
    )
```

```python
import functools
import math

import jax
import jax.numpy as jnp
from jax import lax
from jax.experimental import pallas as pl
from jax.experimental.pallas import tpu as pltpu
from jax.sharding import PartitionSpec as P

BF, F32 = jnp.bfloat16, jnp.float32
MESH = pl.DeviceIdType.MESH
ANY = pl.BlockSpec(memory_space=pl.ANY)
VMEM_LIMIT = 66 * 1024 * 1024 - 2 * 1024 * 1024

UNITS = (("d", 1), ("g", 1), ("u", 1), ("d", 0), ("g", 0), ("u", 0))
WIDE = (("g", 1), ("u", 1), ("g", 0), ("u", 0))
TALL = (("d", 1), ("d", 0))
BLOCKS = 4
TOKEN_BLOCKS = 4


def adamw(w, m, v, g):
    m = 0.9 * m + 0.1 * g
    v = 0.95 * v + 0.05 * g * g
    step = m * lax.rsqrt(v + 1e-8) + 0.1 * w
    return (w - 0.02 * step).astype(BF), m, v


def step_kernel(side, rows, cols, *refs):
    dy_t, a1_t, a0_t = refs[0:3]
    act1, dg1, du1, act0, p0, s0, h1, dy, gate1, up1, down0 = refs[3:14]
    gate1, up1, down0 = gate1.at[1], up1.at[1], down0.at[0]
    w_in, m_in, v_in = refs[14:17], refs[17:20], refs[20:23]
    w_out, m_out, v_out, (dg0, du0) = refs[23:26], refs[26:29], refs[29:32], refs[32:34]
    (gw, gt, r1w, r1t, r2w, r2t, left_buf, right_buf, dh_t, down_buf, h_buf, factor_buf, out_buf, ow, ot, mw, mt, vw, vt, g_full) = refs[34:54]
    (send1, recv1, send2, recv2, left_sem, right_sem, tile_sem, h_sem, factor_sem, tile_out_sem, state_sem, out_sem) = refs[54:]
    rights = {("d", 1): act1, ("g", 1): dg1, ("u", 1): du1, ("d", 0): act0, ("g", 0): dg0, ("u", 0): du0}
    me = lax.axis_index("dp")
    at = (me // side, me % side)
    kinds = ("g", "u", "d")

    def index(x, y):
        return lax.rem(x + side, side) * side + lax.rem(y + side, side)

    def near(axis, by):
        return index(at[0] + by, at[1]) if axis == 0 else index(at[0], at[1] + by)

    steps = {(axis, by): lax.rem(at[axis] + by + side, side) for axis in (0, 1) for by in (-1, 1, 2)}

    def along(axis, by):
        return steps[axis, by]

    right_of, left_of = [near(a, 1) for a in (0, 1)], [near(a, -1) for a in (0, 1)]

    def part(unit, h, s):
        if unit[0] == "d":
            size = g_full.shape[0] // 4
            return (pl.ds((2 * h + s) * size, size), slice(None))
        size = gw.shape[-1] // 4
        return (slice(None), pl.ds((2 * h + s) * size, size))

    def pick(unit):
        if unit[0] == "d":
            n = TALL.index(unit)
            return gt.at[n], r1t.at[n], r2t.at[n]
        n = WIDE.index(unit)
        return gw.at[n], r1w.at[n], r2w.at[n]

    def several(unit, h, i, s):
        g = pick(unit)[0]
        lead = (i, slice(None)) if h == 0 else (slice(None), i)
        return g.at[lead + part(unit, h, s)]

    def single(unit, h, i, j, s):
        g = pick(unit)[0]
        lead = (i, j) if h == 0 else (j, i)
        return g.at[lead + part(unit, h, s)]

    def remote(src, dst, send, recv, to):
        return pltpu.make_async_remote_copy(src_ref=src, dst_ref=dst, send_sem=send, recv_sem=recv, device_id={"dp": to}, device_id_type=MESH)

    sent = []

    def push(src, dst, send, recv, to):
        remote(src(), dst(), send(), recv(), to).start()
        sent.append((src, dst, send, recv, to))

    def arrived(dst, send, recv):
        remote(dst, dst, send, recv, right_of[0]).wait_recv()

    def push1(unit, h, slot, src, dst, to):
        u = UNITS.index(unit)
        push(src, dst, lambda: send1.at[u, h, slot], lambda: recv1.at[u, h, slot], to)

    def push2(unit, h, slot, src, dst, to):
        u = UNITS.index(unit)
        push(src, dst, lambda: send2.at[u, h, slot], lambda: recv2.at[u, h, slot], to)

    def arrived1(unit, h, slot):
        u = UNITS.index(unit)
        dst = pick(unit)[1].at[h, slot] if slot < 6 else pick(unit)[2].at[h, slot - 6]
        arrived(dst, send1.at[u, h, slot], recv1.at[u, h, slot])

    def first(unit, h, slot):
        return lambda: pick(unit)[1].at[h, slot]

    def second(unit, h, slot):
        return lambda: pick(unit)[2].at[h, slot]

    def phase1_send(unit):
        for h in (0, 1):
            far, nxt, prv = along(h, 2), along(h, 1), along(h, -1)
            for slot, i, s, to in ((0, far, 1, right_of[h]), (1, far, 0, left_of[h]), (2, nxt, 0, right_of[h]), (3, prv, 1, left_of[h])):
                push1(unit, h, slot, functools.partial(several, unit, h, i, s), first(unit, h, slot), to)

    def phase1_pass(unit):
        r1 = pick(unit)[1]
        for h in (0, 1):
            for slot, i, s, out, to in ((0, along(h, 1), 1, 4, right_of[h]), (1, along(h, -1), 0, 5, left_of[h])):
                arrived1(unit, h, slot)
                for j in range(side):
                    here = single(unit, h, i, j, s)
                    here[...] = (here[...].astype(F32) + r1[h, slot, j].astype(F32)).astype(BF)
                push1(unit, h, out, functools.partial(several, unit, h, i, s), first(unit, h, out), to)

    def row_sum(unit, h, j, s):
        _, r1, _ = pick(unit)
        one, two = (2, 5) if s == 0 else (4, 3)
        return single(unit, h, at[h], j, s)[...].astype(F32) + r1[h, one, j].astype(F32) + r1[h, two, j].astype(F32)

    def phase2_send(unit):
        for h in (0, 1):
            for slot in (2, 3, 4, 5):
                arrived1(unit, h, slot)
            o = 1 - h
            far, nxt, prv = along(o, 2), along(o, 1), along(o, -1)
            for slot, j, s, to in ((0, far, 1, right_of[o]), (1, far, 0, left_of[o]), (2, nxt, 0, right_of[o]), (3, prv, 1, left_of[o])):
                single(unit, h, at[h], j, s)[...] = row_sum(unit, h, j, s).astype(BF)
                push1(unit, h, 6 + slot, functools.partial(single, unit, h, at[h], j, s), second(unit, h, slot), to)

    def phase2_pass(unit):
        r2 = pick(unit)[2]
        for h in (0, 1):
            o = 1 - h
            for slot, j, s, out, to in ((0, along(o, 1), 1, 4, right_of[o]), (1, along(o, -1), 0, 5, left_of[o])):
                arrived1(unit, h, 6 + slot)
                single(unit, h, at[h], j, s)[...] = (row_sum(unit, h, j, s) + r2[h, slot].astype(F32)).astype(BF)
                push1(unit, h, 6 + out, functools.partial(single, unit, h, at[h], j, s), second(unit, h, out), to)

    def state(unit):
        k = kinds.index(unit[0])
        n = TALL.index(unit) if unit[0] == "d" else WIDE.index(unit)
        own, m, v = (ot, mt, vt) if unit[0] == "d" else (ow, mw, vw)
        return k, own.at[n], m.at[n], v.at[n]

    def state_copies(unit, which=(0, 1, 2)):
        u = UNITS.index(unit)
        k, own, m, v = state(unit)
        layer = unit[1]
        pairs = ((w_in[k].at[layer, me], own), (m_in[k].at[layer], m), (v_in[k].at[layer], v))
        return [pltpu.make_async_copy(*pairs[i], state_sem.at[u, i]) for i in which]

    def result_copies(unit, which=(0, 1, 2)):
        u = UNITS.index(unit)
        k, own, m, v = state(unit)
        layer = unit[1]
        pairs = ((own, w_out[k].at[layer, at[0], at[1]]), (m, m_out[k].at[layer]), (v, v_out[k].at[layer]))
        return [pltpu.make_async_copy(*pairs[i], out_sem.at[u, i]) for i in which]

    def total(unit, h, s):
        _, _, r2 = pick(unit)
        one, two = (2, 5) if s == 0 else (4, 3)
        g = row_sum(unit, h, at[1 - h], s) + r2[h, one].astype(F32) + r2[h, two].astype(F32)
        return g.astype(BF).astype(F32)

    def w_part(unit, h, s):
        k, own, _, _ = state(unit)
        if unit[0] == "d":
            size = own.shape[0] // 4
            start, count = ((2 * h + s) * size, size) if s is not None else (2 * h * size, 2 * size)
            return (pl.ds(start, count), slice(None))
        size = own.shape[1] // 4
        start, count = ((2 * h + s) * size, size) if s is not None else (2 * h * size, 2 * size)
        return (slice(None), pl.ds(start, count))

    def w_single(unit, h, i, j, s):
        k = kinds.index(unit[0])
        lead = (i, j) if h == 0 else (j, i)
        return w_out[k].at[(unit[1],) + lead + w_part(unit, h, s)]

    def w_several(unit, h, i, s):
        k = kinds.index(unit[0])
        lead = (i, slice(None)) if h == 0 else (slice(None), i)
        return w_out[k].at[(unit[1],) + lead + w_part(unit, h, s)]

    def update(unit):
        u = UNITS.index(unit)
        k, own, m, v = state(unit)
        for copy in state_copies(unit):
            copy.wait()
        for h in (0, 1):
            for slot in (2, 3, 4, 5):
                arrived1(unit, h, 6 + slot)
        if unit[0] == "d":
            for h in (0, 1):
                for s in (0, 1):
                    g_full[part(unit, h, s)[0], :] = total(unit, h, s)
            own[...], m[...], v[...] = adamw(own[...].astype(F32), m[...], v[...], g_full[...].T)
        else:
            for h in (0, 1):
                for s in (0, 1):
                    c = part(unit, h, s)
                    own[c], m[c], v[c] = adamw(own[c].astype(F32), m[c], v[c], total(unit, h, s))
        for copy in result_copies(unit):
            copy.start()
        for h in (0, 1):
            o = 1 - h
            src = lambda unit=unit, h=h: state(unit)[1].at[w_part(unit, h, None)]
            dst = functools.partial(w_single, unit, h, at[h], at[o], None)
            push2(unit, h, 0, src, dst, right_of[o])
            push2(unit, h, 1, src, dst, left_of[o])

    def arrived2(unit, h, slot, dst):
        u = UNITS.index(unit)
        arrived(dst, send2.at[u, h, slot], recv2.at[u, h, slot])

    def gather1_pass(unit):
        for h in (0, 1):
            o = 1 - h
            for slot, by, s, to in ((0, -1, 1, right_of[o]), (1, 1, 0, left_of[o])):
                arrived2(unit, h, slot, w_single(unit, h, at[h], along(o, by), None))
                piece = functools.partial(w_single, unit, h, at[h], along(o, by), s)
                push2(unit, h, 2 + slot, piece, piece, to)

    def gather2_send(unit):
        result_copies(unit, (0,))[0].wait()
        for h in (0, 1):
            o = 1 - h
            for slot, s in ((2, 1), (3, 0)):
                arrived2(unit, h, slot, w_single(unit, h, at[h], along(o, 2), s))
            piece = functools.partial(w_several, unit, h, at[h], None)
            push2(unit, h, 4, piece, piece, right_of[h])
            push2(unit, h, 5, piece, piece, left_of[h])

    def gather2_pass(unit):
        for h in (0, 1):
            for slot, by, s, to in ((4, -1, 1, right_of[h]), (5, 1, 0, left_of[h])):
                arrived2(unit, h, slot, w_several(unit, h, along(h, by), None))
                piece = functools.partial(w_several, unit, h, along(h, by), s)
                push2(unit, h, 2 + slot, piece, piece, to)

    def gather2_end(unit):
        for h in (0, 1):
            for slot, s in ((6, 1), (7, 0)):
                arrived2(unit, h, slot, w_several(unit, h, along(h, 2), s))

    width = right_buf.shape[-1]
    count = right_buf.shape[1]

    def fill(src, slot):
        return pltpu.make_async_copy(src, left_buf.at[slot], left_sem.at[slot])

    def right_copy(unit, n, slot):
        columns = pl.ds(pl.multiple_of(n * width, width), width)
        return pltpu.make_async_copy(rights[unit].at[:, :, columns], right_buf_of(slot), right_sem.at[slot])

    def right_buf_of(slot):
        return right_buf.at[pl.ds(slot * TOKEN_BLOCKS, TOKEN_BLOCKS)]

    def gradient(unit, left, then):
        def block(n, _):
            slot = lax.rem(n, 2)

            @pl.when(n < BLOCKS - 1)
            def _():
                right_copy(unit, n + 1, 1 - slot).start()

            if then is not None:

                @pl.when(n == BLOCKS - 1)
                def _():
                    right_copy(then, 0, 1 - slot).start()

            right_copy(unit, n, slot).wait()
            right = right_buf[pl.ds(slot * TOKEN_BLOCKS, TOKEN_BLOCKS)].reshape(TOKEN_BLOCKS * count, width)
            out = jnp.dot(left[...], right, preferred_element_type=F32)
            g = pick(unit)[0]
            if unit[0] == "d":
                for c in range(width // cols):
                    chunk = n * (width // cols) + c
                    g[chunk // side, lax.rem(chunk, side)] = out[:, c * cols : (c + 1) * cols].astype(BF)
            else:
                for x in range(side):
                    for y in range(side):
                        r = (x * side + y) * rows
                        g[x, y, :, pl.ds(pl.multiple_of(n * width, width), width)] = out[r : r + rows].astype(BF)
            return 0

        lax.fori_loop(0, BLOCKS, block, 0)

    def tile(src, t, f, slot):
        return pltpu.make_async_copy(src.at[t, :, pl.ds(f * width, width)], right_buf.at[slot * TOKEN_BLOCKS + f], tile_sem.at[slot, f])

    def tiles(src, t, slot):
        return [tile(src, t, f, slot) for f in range(BLOCKS)]

    def state_tiles(t):
        return [pltpu.make_async_copy(src.at[t], h_buf.at[i], h_sem.at[i]) for i, src in enumerate((h1, dy))]

    def factor_tiles(t, f, slot):
        return [pltpu.make_async_copy(src.at[t, :, pl.ds(f * width, width)], factor_buf.at[slot, i], factor_sem.at[slot, i]) for i, src in enumerate((p0, s0))]

    def result_tiles(t, f, slot):
        return [pltpu.make_async_copy(out_buf.at[slot, i], dst.at[t, :, pl.ds(f * width, width)], tile_out_sem.at[slot, i]) for i, dst in enumerate((dg0, du0))]

    def start(copies):
        for copy in copies:
            copy.start()

    def wait(copies):
        for copy in copies:
            copy.wait()

    def against(buf, slot):
        total = None
        for f in range(BLOCKS):
            term = lax.dot_general(right_buf[slot * TOKEN_BLOCKS + f], buf[:, f * width : (f + 1) * width], (((1,), (1,)), ((), ())), preferred_element_type=F32)
            total = term if total is None else total + term
        return total.astype(BF).astype(F32)

    def between(work):
        start(tiles(du1, 0, 1))
        down = pltpu.make_async_copy(down0, down_buf, left_sem.at[2])

        def block(t, _):
            last = TOKEN_BLOCKS - 1
            start(factor_tiles(t, 0, 0))
            wait(tiles(dg1, t, 0))
            da = against(left_buf.at[0], 0)

            @pl.when(t < last)
            def _():
                start(tiles(dg1, t + 1, 0))

            wait(tiles(du1, t, 1))
            da = da + against(left_buf.at[1], 1)

            @pl.when(t < last)
            def _():
                start(tiles(du1, t + 1, 1))

            wait(state_tiles(t))
            h = h_buf[0].astype(F32)
            da = da.astype(BF).astype(F32)
            scale = lax.rsqrt(jnp.mean(h * h, -1, keepdims=True) + 1e-6)
            inner = jnp.sum(da * h, -1, keepdims=True)
            back = da * scale - h * (scale * scale * scale * inner / h.shape[-1])
            dh = h_buf[1].astype(F32) + back.astype(BF).astype(F32)
            dh_t[:, pl.ds(pl.multiple_of(t * count, count), count)] = dh.T.astype(BF)
            dh = dh.astype(BF)

            @pl.when(t < last)
            def _():
                start(state_tiles(t + 1))

            for f in range(BLOCKS):
                slot = f % 2
                if f + 1 < BLOCKS:
                    start(factor_tiles(t, f + 1, 1 - slot))
                d = lax.dot_general(dh, down_buf[f * width : (f + 1) * width], (((1,), (1,)), ((), ())), preferred_element_type=F32).astype(BF).astype(F32)
                wait(factor_tiles(t, f, slot))
                if f >= 2:
                    wait(result_tiles(t, f - 2, slot))
                for i in (0, 1):
                    out_buf[slot, i] = (d * factor_buf[slot, i]).astype(BF)
                start(result_tiles(t, f, slot))
            for f in (BLOCKS - 2, BLOCKS - 1):
                wait(result_tiles(t, f, f % 2))
            for k in range(TOKEN_BLOCKS):

                @pl.when(t == k)
                def _():
                    work(k)

            return 0

        wait([fill(gate1, 0), fill(up1, 1), down])
        lax.fori_loop(0, TOKEN_BLOCKS, block, 0)

    start([fill(dy_t, 0), right_copy(UNITS[0], 0, 0), fill(a1_t, 1), pltpu.make_async_copy(down0, down_buf, left_sem.at[2])])
    start(state_tiles(0))
    for unit in UNITS:
        start(state_copies(unit))
    barrier = pltpu.get_barrier_semaphore()
    for a in (0, 1):
        for to in (left_of[a], right_of[a]):
            pl.semaphore_signal(barrier, inc=1, device_id={"dp": to}, device_id_type=MESH)
    pl.semaphore_wait(barrier, 4)

    stages = (phase1_send, phase1_pass, phase2_send, phase2_pass, update, gather1_pass, gather2_send, gather2_pass, gather2_end)
    begins = dict(zip(UNITS, (0, 1, 2, 3 + TOKEN_BLOCKS, 4 + TOKEN_BLOCKS, 5 + TOKEN_BLOCKS), strict=True))

    def communicate(t):
        for unit in UNITS:
            if 0 <= t - begins[unit] < len(stages):
                stages[t - begins[unit]](unit)

    d1, g1, u1, d0, g0, u0 = UNITS
    fill(dy_t, 0).wait()
    gradient(d1, left_buf.at[0], g1)
    fill(gate1, 0).start()
    communicate(0)
    fill(a1_t, 1).wait()
    gradient(g1, left_buf.at[1], u1)
    communicate(1)
    gradient(u1, left_buf.at[1], None)
    fill(up1, 1).start()
    start(tiles(dg1, 0, 0))
    communicate(2)
    between(lambda k: communicate(3 + k))
    fill(a0_t, 0).start()
    right_copy(d0, 0, 0).start()
    gradient(d0, dh_t, g0)
    communicate(begins[d0])
    fill(a0_t, 0).wait()
    gradient(g0, left_buf.at[0], u0)
    communicate(begins[g0])
    gradient(u0, left_buf.at[0], None)
    for t in range(begins[u0], begins[u0] + len(stages)):
        communicate(t)
    for unit in UNITS:
        wait(result_copies(unit, (1, 2)))
    for src, dst, send, recv, to in sent:
        remote(src(), dst(), send(), recv(), to).wait_send()


def reduce_step_gather(n, dy_t, a1_t, a0_t, act1, dg1, du1, act0, p0, s0, h1, dy, weights, m, v):
    side = math.isqrt(n)
    layers, rows, ff = m[0].shape
    cols, d = m[2].shape[1:]
    blocked = [w.reshape(layers, n, -1, w.shape[-1]) for w in weights]
    half, part = ff // 2, ff // 4
    width = ff // BLOCKS
    tokens = dy_t.shape[1]
    count = tokens // TOKEN_BLOCKS
    tiled = [t.reshape(TOKEN_BLOCKS, count, t.shape[-1]) for t in (act1, dg1, du1, act0, p0, s0, h1, dy)]
    out_shape = (
        [jax.ShapeDtypeStruct((layers, side, side, rows, ff), BF)] * 2
        + [jax.ShapeDtypeStruct((layers, side, side, cols, d), BF)]
        + [jax.ShapeDtypeStruct(t.shape, F32) for t in (*m, *v)]
        + [jax.ShapeDtypeStruct((TOKEN_BLOCKS, count, ff), BF)] * 2
    )
    nw, nt, nu = len(WIDE), len(TALL), len(UNITS)
    dma = pltpu.SemaphoreType.DMA
    out = pl.pallas_call(
        functools.partial(step_kernel, side, rows, cols),
        out_shape=out_shape,
        in_specs=[ANY] * 23,
        out_specs=[ANY] * 11,
        scratch_shapes=[
            pltpu.VMEM((nw, side, side, rows, ff), BF),
            pltpu.VMEM((nt, side, side, d, cols), BF),
            pltpu.VMEM((nw, 2, 6, side, rows, part), BF),
            pltpu.VMEM((nt, 2, 6, side, d // 4, cols), BF),
            pltpu.VMEM((nw, 2, 6, rows, part), BF),
            pltpu.VMEM((nt, 2, 6, d // 4, cols), BF),
            pltpu.VMEM((2, d, tokens), BF),
            pltpu.VMEM((2 * TOKEN_BLOCKS, count, width), BF),
            pltpu.VMEM((d, tokens), BF),
            pltpu.VMEM((ff, d), BF),
            pltpu.VMEM((2, count, d), BF),
            pltpu.VMEM((2, 2, count, width), F32),
            pltpu.VMEM((2, 2, count, width), BF),
            pltpu.VMEM((nw, rows, ff), BF),
            pltpu.VMEM((nt, cols, d), BF),
            pltpu.VMEM((nw, rows, ff), F32),
            pltpu.VMEM((nt, cols, d), F32),
            pltpu.VMEM((nw, rows, ff), F32),
            pltpu.VMEM((nt, cols, d), F32),
            pltpu.VMEM((d, cols), F32),
            dma((nu, 2, 12)),
            dma((nu, 2, 12)),
            dma((nu, 2, 8)),
            dma((nu, 2, 8)),
            dma((3,)),
            dma((2,)),
            dma((2, BLOCKS)),
            dma((2,)),
            dma((2, 2)),
            dma((2, 2)),
            dma((nu, 3)),
            dma((nu, 3)),
        ],
        compiler_params=pltpu.CompilerParams(collective_id=0, has_side_effects=True, vmem_limit_bytes=VMEM_LIMIT),
        name="reduce_step_gather",
    )(dy_t, a1_t, a0_t, *tiled, *weights, *blocked, *m, *v)
    return tuple(w.reshape(layers, -1, w.shape[-1]) for w in out[:3]) + tuple(out[3:9])


def front_kernel(x, dy, *refs):
    weights, (act0, act1, dg1, du1, p0, s0, h1, a0_t, a1_t, dy_t), bufs, a_buf, sem = refs[:3], refs[3:13], refs[13:16], refs[16], refs[17]
    first = pl.program_id(0) == 0
    ff = act0.shape[1]
    width = ff // BLOCKS

    def copy(layer, k):
        return pltpu.make_async_copy(weights[k].at[layer], bufs[k].at[layer], sem.at[layer, k])

    def normed(h, t_ref):
        wide = h[...].astype(F32)
        a = wide * lax.rsqrt(jnp.mean(wide * wide, -1, keepdims=True) + 1e-6)
        a_buf[...] = a.astype(BF)
        t_ref[...] = a.T.astype(BF)

    @pl.when(first)
    def _():
        for layer in (0, 1):
            for k in range(3):
                copy(layer, k).start()

    normed(x, a0_t)
    dy_t[...] = dy[...].astype(F32).T.astype(BF)

    def ready(layer):
        @pl.when(first)
        def _():
            for k in range(3):
                copy(layer, k).wait()

    ready(0)
    for f in range(BLOCKS):
        c = slice(f * width, (f + 1) * width)
        gate = jnp.dot(a_buf[...], bufs[0][0, :, c], preferred_element_type=F32)
        up = jnp.dot(a_buf[...], bufs[1][0, :, c], preferred_element_type=F32)
        sig = jax.nn.sigmoid(gate)
        silu = gate * sig
        act0[:, c] = (silu * up).astype(BF)
        p0[:, c] = up * (sig + silu * (1 - sig))
        s0[:, c] = silu
    h1[...] = (x[...].astype(F32) + jnp.dot(act0[...], bufs[2][0], preferred_element_type=F32).astype(BF).astype(F32)).astype(BF)
    normed(h1, a1_t)
    ready(1)
    for f in range(BLOCKS):
        c = slice(f * width, (f + 1) * width)
        gate = jnp.dot(a_buf[...], bufs[0][1, :, c], preferred_element_type=F32)
        up = jnp.dot(a_buf[...], bufs[1][1, :, c], preferred_element_type=F32)
        d = lax.dot_general(dy[...], bufs[2][1, c, :], (((1,), (1,)), ((), ())), preferred_element_type=F32).astype(BF).astype(F32)
        sig = jax.nn.sigmoid(gate)
        silu = gate * sig
        act1[:, c] = (silu * up).astype(BF)
        dg1[:, c] = (d * up * (sig + silu * (1 - sig))).astype(BF)
        du1[:, c] = (d * silu).astype(BF)


def front(x, dy, weights):
    tokens, d = x.shape
    layers, _, ff = weights[0].shape
    count = tokens // TOKEN_BLOCKS
    row = lambda n: pl.BlockSpec((count, n), lambda t: (t, 0))
    column = pl.BlockSpec((d, count), lambda t: (0, t))
    shape = jax.ShapeDtypeStruct
    return pl.pallas_call(
        front_kernel,
        grid=(TOKEN_BLOCKS,),
        out_shape=[shape((tokens, ff), BF)] * 4 + [shape((tokens, ff), F32)] * 2 + [shape((tokens, d), BF)] + [shape((d, tokens), BF)] * 3,
        in_specs=[row(d)] * 2 + [ANY] * 3,
        out_specs=[row(ff)] * 6 + [row(d)] + [column] * 3,
        scratch_shapes=[pltpu.VMEM(w.shape, BF) for w in weights] + [pltpu.VMEM((count, d), BF), pltpu.SemaphoreType.DMA((layers, 3))],
        compiler_params=pltpu.CompilerParams(vmem_limit_bytes=VMEM_LIMIT, dimension_semantics=("arbitrary",)),
        name="front",
    )(x, dy, *weights)


def solution(mesh):
    n = mesh.shape["dp"]

    def step(x, dy, *arrays):
        weights, m, v = (arrays[i : i + 3] for i in (0, 3, 6))
        act0, act1, dg1, du1, p0, s0, h1, a0_t, a1_t, dy_t = front(x[0], dy[0], weights)
        return reduce_step_gather(n, dy_t, a1_t, a0_t, act1, dg1, du1, act0, p0, s0, h1, dy[0], weights, m, v)

    rows = P(None, "dp", None)
    return jax.shard_map(
        step,
        mesh=mesh,
        in_specs=(P(("rep", "dp"), None, None),) * 2 + (P(None, None, None),) * 3 + (rows,) * 6,
        out_specs=(P("rep", None, None),) * 3 + (P("rep", "dp", None),) * 6,
        check_vma=False,
    )
```

```python
import functools
import math

import jax
import jax.numpy as jnp
from jax import lax
from jax.experimental import pallas as pl
from jax.experimental.pallas import tpu as pltpu
from jax.sharding import PartitionSpec as P

BF, F32 = jnp.bfloat16, jnp.float32
MESH = pl.DeviceIdType.MESH
ANY = pl.BlockSpec(memory_space=pl.ANY)
VMEM_LIMIT = 66 * 1024 * 1024 - 2 * 1024 * 1024

UNITS = (("d", 1), ("g", 1), ("u", 1), ("d", 0), ("g", 0), ("u", 0))
WIDE = (("g", 1), ("u", 1), ("g", 0), ("u", 0))
TALL = (("d", 1), ("d", 0))
BLOCKS = 4
TOKEN_BLOCKS = 4
FRONT_BLOCKS = 8

ORDER = (
    ((0, 0),),
    ((0, 1), (1, 0)),
    ((0, 2), (1, 1)),
    ((2, 0), (1, 2)),
    ((3, 0), (2, 1)),
    ((4, 0), (3, 1), (2, 2)),
    ((5, 0), (4, 1), (3, 2)),
    ((5, 1), (4, 2), (6, 0)),
    ((5, 2), (6, 1)),
    (),
    ((7, 0), (6, 2)),
    ((0, 3), (8, 0), (7, 1)),
    ((0, 4), (1, 3), (7, 2)),
    ((0, 5), (1, 4), (8, 1), (2, 3), (8, 2), (1, 5), (2, 4), (3, 3), (2, 5), (3, 4), (4, 3), (3, 5), (4, 4), (5, 3), (4, 5), (5, 4), (6, 3), (5, 5), (6, 4), (7, 3), (6, 5), (7, 4), (8, 3), (7, 5), (8, 4), (8, 5)),
)


def adamw(w, m, v, g):
    m = 0.9 * m + 0.1 * g
    v = 0.95 * v + 0.05 * g * g
    step = m * lax.rsqrt(v + 1e-8) + 0.1 * w
    return (w - 0.02 * step).astype(BF), m, v


def step_kernel(side, rows, cols, *refs):
    dy_t, a1_t, a0_t = refs[0:3]
    act1, dg1, du1, act0, p0, s0, h1, dy, gate1, up1, down0 = refs[3:14]
    gate1, up1, down0 = gate1.at[1], up1.at[1], down0.at[0]
    w_in, m_in, v_in = refs[14:17], refs[17:20], refs[20:23]
    w_out, m_out, v_out, (dg0, du0) = refs[23:26], refs[26:29], refs[29:32], refs[32:34]
    (gw, gt, r1w, r1t, r2w, r2t, left_buf, right_buf, dh_t, down_buf, h_buf, factor_buf, out_buf, ow, ot, mw, mt, vw, vt, g_full) = refs[34:54]
    (send1, recv1, send2, recv2, left_sem, right_sem, tile_sem, h_sem, factor_sem, tile_out_sem, state_sem, out_sem) = refs[54:]
    rights = {("d", 1): act1, ("g", 1): dg1, ("u", 1): du1, ("d", 0): act0, ("g", 0): dg0, ("u", 0): du0}
    me = lax.axis_index("dp")
    at = (me // side, me % side)
    kinds = ("g", "u", "d")

    def index(x, y):
        return lax.rem(x + side, side) * side + lax.rem(y + side, side)

    def near(axis, by):
        return index(at[0] + by, at[1]) if axis == 0 else index(at[0], at[1] + by)

    steps = {(axis, by): lax.rem(at[axis] + by + side, side) for axis in (0, 1) for by in (-1, 1, 2)}

    def along(axis, by):
        return steps[axis, by]

    right_of, left_of = [near(a, 1) for a in (0, 1)], [near(a, -1) for a in (0, 1)]

    def part(unit, h, s):
        if unit[0] == "d":
            size = g_full.shape[0] // 4
            return (pl.ds((2 * h + s) * size, size), slice(None))
        size = gw.shape[-1] // 4
        return (slice(None), pl.ds((2 * h + s) * size, size))

    def pick(unit):
        if unit[0] == "d":
            n = TALL.index(unit)
            return gt.at[n], r1t.at[n], r2t.at[n]
        n = WIDE.index(unit)
        return gw.at[n], r1w.at[n], r2w.at[n]

    def several(unit, h, i, s):
        g = pick(unit)[0]
        lead = (i, slice(None)) if h == 0 else (slice(None), i)
        return g.at[lead + part(unit, h, s)]

    def single(unit, h, i, j, s):
        g = pick(unit)[0]
        lead = (i, j) if h == 0 else (j, i)
        return g.at[lead + part(unit, h, s)]

    def remote(src, dst, send, recv, to):
        return pltpu.make_async_remote_copy(src_ref=src, dst_ref=dst, send_sem=send, recv_sem=recv, device_id={"dp": to}, device_id_type=MESH)

    sent = []

    def push(src, dst, send, recv, to):
        remote(src(), dst(), send(), recv(), to).start()
        sent.append((src, dst, send, recv, to))

    def arrived(dst, send, recv):
        remote(dst, dst, send, recv, right_of[0]).wait_recv()

    def push1(unit, h, slot, src, dst, to):
        u = UNITS.index(unit)
        push(src, dst, lambda: send1.at[u, h, slot], lambda: recv1.at[u, h, slot], to)

    def push2(unit, h, slot, src, dst, to):
        u = UNITS.index(unit)
        push(src, dst, lambda: send2.at[u, h, slot], lambda: recv2.at[u, h, slot], to)

    def arrived1(unit, h, slot):
        u = UNITS.index(unit)
        dst = pick(unit)[1].at[h, slot] if slot < 6 else pick(unit)[2].at[h, slot - 6]
        arrived(dst, send1.at[u, h, slot], recv1.at[u, h, slot])

    def first(unit, h, slot):
        return lambda: pick(unit)[1].at[h, slot]

    def second(unit, h, slot):
        return lambda: pick(unit)[2].at[h, slot]

    def phase1_send(unit):
        for h in (0, 1):
            far, nxt, prv = along(h, 2), along(h, 1), along(h, -1)
            for slot, i, s, to in ((0, far, 1, right_of[h]), (1, far, 0, left_of[h]), (2, nxt, 0, right_of[h]), (3, prv, 1, left_of[h])):
                push1(unit, h, slot, functools.partial(several, unit, h, i, s), first(unit, h, slot), to)

    def phase1_pass(unit):
        r1 = pick(unit)[1]
        for h in (0, 1):
            for slot, i, s, out, to in ((0, along(h, 1), 1, 4, right_of[h]), (1, along(h, -1), 0, 5, left_of[h])):
                arrived1(unit, h, slot)
                for j in range(side):
                    here = single(unit, h, i, j, s)
                    here[...] = (here[...].astype(F32) + r1[h, slot, j].astype(F32)).astype(BF)
                push1(unit, h, out, functools.partial(several, unit, h, i, s), first(unit, h, out), to)

    def row_sum(unit, h, j, s):
        _, r1, _ = pick(unit)
        one, two = (2, 5) if s == 0 else (4, 3)
        return single(unit, h, at[h], j, s)[...].astype(F32) + r1[h, one, j].astype(F32) + r1[h, two, j].astype(F32)

    def phase2_send(unit):
        for h in (0, 1):
            for slot in (2, 3, 4, 5):
                arrived1(unit, h, slot)
            o = 1 - h
            far, nxt, prv = along(o, 2), along(o, 1), along(o, -1)
            for slot, j, s, to in ((0, far, 1, right_of[o]), (1, far, 0, left_of[o]), (2, nxt, 0, right_of[o]), (3, prv, 1, left_of[o])):
                single(unit, h, at[h], j, s)[...] = row_sum(unit, h, j, s).astype(BF)
                push1(unit, h, 6 + slot, functools.partial(single, unit, h, at[h], j, s), second(unit, h, slot), to)

    def phase2_pass(unit):
        r2 = pick(unit)[2]
        for h in (0, 1):
            o = 1 - h
            for slot, j, s, out, to in ((0, along(o, 1), 1, 4, right_of[o]), (1, along(o, -1), 0, 5, left_of[o])):
                arrived1(unit, h, 6 + slot)
                single(unit, h, at[h], j, s)[...] = (row_sum(unit, h, j, s) + r2[h, slot].astype(F32)).astype(BF)
                push1(unit, h, 6 + out, functools.partial(single, unit, h, at[h], j, s), second(unit, h, out), to)

    def state(unit):
        k = kinds.index(unit[0])
        n = TALL.index(unit) if unit[0] == "d" else WIDE.index(unit)
        own, m, v = (ot, mt, vt) if unit[0] == "d" else (ow, mw, vw)
        return k, own.at[n], m.at[n], v.at[n]

    def state_copies(unit, which=(0, 1, 2)):
        u = UNITS.index(unit)
        k, own, m, v = state(unit)
        layer = unit[1]
        pairs = ((w_in[k].at[layer, me], own), (m_in[k].at[layer], m), (v_in[k].at[layer], v))
        return [pltpu.make_async_copy(*pairs[i], state_sem.at[u, i]) for i in which]

    def result_copies(unit, which=(0, 1, 2)):
        u = UNITS.index(unit)
        k, own, m, v = state(unit)
        layer = unit[1]
        pairs = ((own, w_out[k].at[layer, at[0], at[1]]), (m, m_out[k].at[layer]), (v, v_out[k].at[layer]))
        return [pltpu.make_async_copy(*pairs[i], out_sem.at[u, i]) for i in which]

    def total(unit, h, s):
        _, _, r2 = pick(unit)
        one, two = (2, 5) if s == 0 else (4, 3)
        g = row_sum(unit, h, at[1 - h], s) + r2[h, one].astype(F32) + r2[h, two].astype(F32)
        return g.astype(BF).astype(F32)

    def w_part(unit, h, s):
        k, own, _, _ = state(unit)
        if unit[0] == "d":
            size = own.shape[0] // 4
            start, count = ((2 * h + s) * size, size) if s is not None else (2 * h * size, 2 * size)
            return (pl.ds(start, count), slice(None))
        size = own.shape[1] // 4
        start, count = ((2 * h + s) * size, size) if s is not None else (2 * h * size, 2 * size)
        return (slice(None), pl.ds(start, count))

    def w_single(unit, h, i, j, s):
        k = kinds.index(unit[0])
        lead = (i, j) if h == 0 else (j, i)
        return w_out[k].at[(unit[1],) + lead + w_part(unit, h, s)]

    def w_several(unit, h, i, s):
        k = kinds.index(unit[0])
        lead = (i, slice(None)) if h == 0 else (slice(None), i)
        return w_out[k].at[(unit[1],) + lead + w_part(unit, h, s)]

    def update(unit):
        u = UNITS.index(unit)
        k, own, m, v = state(unit)
        for copy in state_copies(unit):
            copy.wait()
        for h in (0, 1):
            for slot in (2, 3, 4, 5):
                arrived1(unit, h, 6 + slot)
        if unit[0] == "d":
            for h in (0, 1):
                for s in (0, 1):
                    g_full[part(unit, h, s)[0], :] = total(unit, h, s)
            own[...], m[...], v[...] = adamw(own[...].astype(F32), m[...], v[...], g_full[...].T)
        else:
            for h in (0, 1):
                for s in (0, 1):
                    c = part(unit, h, s)
                    own[c], m[c], v[c] = adamw(own[c].astype(F32), m[c], v[c], total(unit, h, s))
        for copy in result_copies(unit):
            copy.start()
        for h in (0, 1):
            o = 1 - h
            src = lambda unit=unit, h=h: state(unit)[1].at[w_part(unit, h, None)]
            dst = functools.partial(w_single, unit, h, at[h], at[o], None)
            push2(unit, h, 0, src, dst, right_of[o])
            push2(unit, h, 1, src, dst, left_of[o])

    def arrived2(unit, h, slot, dst):
        u = UNITS.index(unit)
        arrived(dst, send2.at[u, h, slot], recv2.at[u, h, slot])

    def gather1_pass(unit):
        for h in (0, 1):
            o = 1 - h
            for slot, by, s, to in ((0, -1, 1, right_of[o]), (1, 1, 0, left_of[o])):
                arrived2(unit, h, slot, w_single(unit, h, at[h], along(o, by), None))
                piece = functools.partial(w_single, unit, h, at[h], along(o, by), s)
                push2(unit, h, 2 + slot, piece, piece, to)

    def gather2_send(unit):
        result_copies(unit, (0,))[0].wait()
        for h in (0, 1):
            o = 1 - h
            for slot, s in ((2, 1), (3, 0)):
                arrived2(unit, h, slot, w_single(unit, h, at[h], along(o, 2), s))
            piece = functools.partial(w_several, unit, h, at[h], None)
            push2(unit, h, 4, piece, piece, right_of[h])
            push2(unit, h, 5, piece, piece, left_of[h])

    def gather2_pass(unit):
        for h in (0, 1):
            for slot, by, s, to in ((4, -1, 1, right_of[h]), (5, 1, 0, left_of[h])):
                arrived2(unit, h, slot, w_several(unit, h, along(h, by), None))
                piece = functools.partial(w_several, unit, h, along(h, by), s)
                push2(unit, h, 2 + slot, piece, piece, to)

    def gather2_end(unit):
        for h in (0, 1):
            for slot, s in ((6, 1), (7, 0)):
                arrived2(unit, h, slot, w_several(unit, h, along(h, 2), s))

    width = right_buf.shape[-1]
    count = right_buf.shape[1]

    def fill(src, slot):
        return pltpu.make_async_copy(src, left_buf.at[slot], left_sem.at[slot])

    def right_copy(unit, n, slot):
        columns = pl.ds(pl.multiple_of(n * width, width), width)
        return pltpu.make_async_copy(rights[unit].at[:, :, columns], right_buf_of(slot), right_sem.at[slot])

    def right_buf_of(slot):
        return right_buf.at[pl.ds(slot * TOKEN_BLOCKS, TOKEN_BLOCKS)]

    def gradient(unit, left, then):
        def block(n, _):
            slot = lax.rem(n, 2)

            @pl.when(n < BLOCKS - 1)
            def _():
                right_copy(unit, n + 1, 1 - slot).start()

            if then is not None:

                @pl.when(n == BLOCKS - 1)
                def _():
                    right_copy(then, 0, 1 - slot).start()

            right_copy(unit, n, slot).wait()
            right = right_buf[pl.ds(slot * TOKEN_BLOCKS, TOKEN_BLOCKS)].reshape(TOKEN_BLOCKS * count, width)
            out = jnp.dot(left[...], right, preferred_element_type=F32)
            g = pick(unit)[0]
            if unit[0] == "d":
                for c in range(width // cols):
                    chunk = n * (width // cols) + c
                    g[chunk // side, lax.rem(chunk, side)] = out[:, c * cols : (c + 1) * cols].astype(BF)
            else:
                for x in range(side):
                    for y in range(side):
                        r = (x * side + y) * rows
                        g[x, y, :, pl.ds(pl.multiple_of(n * width, width), width)] = out[r : r + rows].astype(BF)
            return 0

        lax.fori_loop(0, BLOCKS, block, 0)

    def tile(src, t, f, slot):
        return pltpu.make_async_copy(src.at[t, :, pl.ds(f * width, width)], right_buf.at[slot * TOKEN_BLOCKS + f], tile_sem.at[slot, f])

    def tiles(src, t, slot):
        return [tile(src, t, f, slot) for f in range(BLOCKS)]

    def state_tiles(t):
        return [pltpu.make_async_copy(src.at[t], h_buf.at[i], h_sem.at[i]) for i, src in enumerate((h1, dy))]

    def factor_tiles(t, f, slot):
        return [pltpu.make_async_copy(src.at[t, :, pl.ds(f * width, width)], factor_buf.at[slot, i], factor_sem.at[slot, i]) for i, src in enumerate((p0, s0))]

    def result_tiles(t, f, slot):
        return [pltpu.make_async_copy(out_buf.at[slot, i], dst.at[t, :, pl.ds(f * width, width)], tile_out_sem.at[slot, i]) for i, dst in enumerate((dg0, du0))]

    def start(copies):
        for copy in copies:
            copy.start()

    def wait(copies):
        for copy in copies:
            copy.wait()

    def against(buf, slot):
        left = jnp.concatenate([right_buf[slot * TOKEN_BLOCKS + f] for f in range(BLOCKS)], axis=1)
        return lax.dot_general(left, buf[...], (((1,), (1,)), ((), ())), preferred_element_type=F32).astype(BF).astype(F32)

    def at_block(t, work, part):
        for k in range(TOKEN_BLOCKS):

            @pl.when(t == k)
            def _():
                work(2 * k + part)

    def between(work):
        start(tiles(du1, 0, 1))
        down = pltpu.make_async_copy(down0, down_buf, left_sem.at[2])

        def block(t, _):
            last = TOKEN_BLOCKS - 1
            start(factor_tiles(t, 0, 0))
            wait(tiles(dg1, t, 0))
            da = against(left_buf.at[0], 0)

            @pl.when(t < last)
            def _():
                start(tiles(dg1, t + 1, 0))

            wait(tiles(du1, t, 1))
            da = da + against(left_buf.at[1], 1)

            @pl.when(t < last)
            def _():
                start(tiles(du1, t + 1, 1))

            wait(state_tiles(t))
            h = h_buf[0].astype(F32)
            da = da.astype(BF).astype(F32)
            scale = lax.rsqrt(jnp.mean(h * h, -1, keepdims=True) + 1e-6)
            inner = jnp.sum(da * h, -1, keepdims=True)
            back = da * scale - h * (scale * scale * scale * inner / h.shape[-1])
            dh = h_buf[1].astype(F32) + back.astype(BF).astype(F32)
            dh_t[:, pl.ds(pl.multiple_of(t * count, count), count)] = dh.T.astype(BF)
            dh = dh.astype(BF)

            @pl.when(t < last)
            def _():
                start(state_tiles(t + 1))

            at_block(t, work, 0)
            for f in range(BLOCKS):
                slot = f % 2
                if f + 1 < BLOCKS:
                    start(factor_tiles(t, f + 1, 1 - slot))
                d = lax.dot_general(dh, down_buf[f * width : (f + 1) * width], (((1,), (1,)), ((), ())), preferred_element_type=F32).astype(BF).astype(F32)
                wait(factor_tiles(t, f, slot))
                if f >= 2:
                    wait(result_tiles(t, f - 2, slot))
                for i in (0, 1):
                    out_buf[slot, i] = (d * factor_buf[slot, i]).astype(BF)
                start(result_tiles(t, f, slot))
            for f in (BLOCKS - 2, BLOCKS - 1):
                wait(result_tiles(t, f, f % 2))
            at_block(t, work, 1)
            return 0

        wait([fill(gate1, 0), fill(up1, 1), down])
        lax.fori_loop(0, TOKEN_BLOCKS, block, 0)

    start([fill(dy_t, 0), right_copy(UNITS[0], 0, 0), fill(a1_t, 1), pltpu.make_async_copy(down0, down_buf, left_sem.at[2])])
    start(state_tiles(0))
    for unit in UNITS:
        start(state_copies(unit))
    barrier = pltpu.get_barrier_semaphore()
    for a in (0, 1):
        for to in (left_of[a], right_of[a]):
            pl.semaphore_signal(barrier, inc=1, device_id={"dp": to}, device_id_type=MESH)
    pl.semaphore_wait(barrier, 4)

    stages = (phase1_send, phase1_pass, phase2_send, phase2_pass, update, gather1_pass, gather2_send, gather2_pass, gather2_end)

    def communicate(t):
        for stage, unit in ORDER[t]:
            stages[stage](UNITS[unit])

    d1, g1, u1, d0, g0, u0 = UNITS
    fill(dy_t, 0).wait()
    gradient(d1, left_buf.at[0], g1)
    fill(gate1, 0).start()
    communicate(0)
    fill(a1_t, 1).wait()
    gradient(g1, left_buf.at[1], u1)
    communicate(1)
    gradient(u1, left_buf.at[1], None)
    fill(up1, 1).start()
    start(tiles(dg1, 0, 0))
    communicate(2)
    between(lambda k: communicate(3 + k))
    fill(a0_t, 0).start()
    right_copy(d0, 0, 0).start()
    gradient(d0, dh_t, g0)
    communicate(3 + 2 * TOKEN_BLOCKS)
    fill(a0_t, 0).wait()
    gradient(g0, left_buf.at[0], u0)
    communicate(4 + 2 * TOKEN_BLOCKS)
    gradient(u0, left_buf.at[0], None)
    communicate(5 + 2 * TOKEN_BLOCKS)
    for unit in UNITS:
        wait(result_copies(unit, (1, 2)))
    for src, dst, send, recv, to in sent:
        remote(src(), dst(), send(), recv(), to).wait_send()


def reduce_step_gather(n, dy_t, a1_t, a0_t, act1, dg1, du1, act0, p0, s0, h1, dy, weights, m, v):
    side = math.isqrt(n)
    layers, rows, ff = m[0].shape
    cols, d = m[2].shape[1:]
    blocked = [w.reshape(layers, n, -1, w.shape[-1]) for w in weights]
    half, part = ff // 2, ff // 4
    width = ff // BLOCKS
    tokens = dy_t.shape[1]
    count = tokens // TOKEN_BLOCKS
    tiled = [t.reshape(TOKEN_BLOCKS, count, t.shape[-1]) for t in (act1, dg1, du1, act0, p0, s0, h1, dy)]
    out_shape = (
        [jax.ShapeDtypeStruct((layers, side, side, rows, ff), BF)] * 2
        + [jax.ShapeDtypeStruct((layers, side, side, cols, d), BF)]
        + [jax.ShapeDtypeStruct(t.shape, F32) for t in (*m, *v)]
        + [jax.ShapeDtypeStruct((TOKEN_BLOCKS, count, ff), BF)] * 2
    )
    nw, nt, nu = len(WIDE), len(TALL), len(UNITS)
    dma = pltpu.SemaphoreType.DMA
    out = pl.pallas_call(
        functools.partial(step_kernel, side, rows, cols),
        out_shape=out_shape,
        in_specs=[ANY] * 23,
        out_specs=[ANY] * 11,
        scratch_shapes=[
            pltpu.VMEM((nw, side, side, rows, ff), BF),
            pltpu.VMEM((nt, side, side, d, cols), BF),
            pltpu.VMEM((nw, 2, 6, side, rows, part), BF),
            pltpu.VMEM((nt, 2, 6, side, d // 4, cols), BF),
            pltpu.VMEM((nw, 2, 6, rows, part), BF),
            pltpu.VMEM((nt, 2, 6, d // 4, cols), BF),
            pltpu.VMEM((2, d, tokens), BF),
            pltpu.VMEM((2 * TOKEN_BLOCKS, count, width), BF),
            pltpu.VMEM((d, tokens), BF),
            pltpu.VMEM((ff, d), BF),
            pltpu.VMEM((2, count, d), BF),
            pltpu.VMEM((2, 2, count, width), F32),
            pltpu.VMEM((2, 2, count, width), BF),
            pltpu.VMEM((nw, rows, ff), BF),
            pltpu.VMEM((nt, cols, d), BF),
            pltpu.VMEM((nw, rows, ff), F32),
            pltpu.VMEM((nt, cols, d), F32),
            pltpu.VMEM((nw, rows, ff), F32),
            pltpu.VMEM((nt, cols, d), F32),
            pltpu.VMEM((d, cols), F32),
            dma((nu, 2, 12)),
            dma((nu, 2, 12)),
            dma((nu, 2, 8)),
            dma((nu, 2, 8)),
            dma((3,)),
            dma((2,)),
            dma((2, BLOCKS)),
            dma((2,)),
            dma((2, 2)),
            dma((2, 2)),
            dma((nu, 3)),
            dma((nu, 3)),
        ],
        compiler_params=pltpu.CompilerParams(collective_id=0, has_side_effects=True, vmem_limit_bytes=VMEM_LIMIT),
        name="reduce_step_gather",
    )(dy_t, a1_t, a0_t, *tiled, *weights, *blocked, *m, *v)
    return tuple(w.reshape(layers, -1, w.shape[-1]) for w in out[:3]) + tuple(out[3:9])


def logistic(x):
    return 0.5 + 0.5 * jnp.tanh(0.5 * x)


def front_kernel(x, dy, *refs):
    weights, (act0, act1, dg1, du1, p0, s0, h1, a0_t, a1_t, dy_t), bufs, a_buf, sem = refs[:3], refs[3:13], refs[13:16], refs[16], refs[17]
    first = pl.program_id(0) == 0
    ff = act0.shape[1]
    width = ff // BLOCKS

    def copy(layer, k):
        return pltpu.make_async_copy(weights[k].at[layer], bufs[k].at[layer], sem.at[layer, k])

    def normed(h, t_ref):
        wide = h[...].astype(F32)
        a = wide * lax.rsqrt(jnp.mean(wide * wide, -1, keepdims=True) + 1e-6)
        a_buf[...] = a.astype(BF)
        t_ref[...] = a.T.astype(BF)

    @pl.when(first)
    def _():
        for layer in (0, 1):
            for k in range(3):
                copy(layer, k).start()

    normed(x, a0_t)
    dy_t[...] = dy[...].astype(F32).T.astype(BF)

    def ready(layer, *which):
        @pl.when(first)
        def _():
            for k in which:
                copy(layer, k).wait()

    ready(0, 0, 1)
    for f in range(BLOCKS):
        c = slice(f * width, (f + 1) * width)
        gate = jnp.dot(a_buf[...], bufs[0][0, :, c], preferred_element_type=F32)
        up = jnp.dot(a_buf[...], bufs[1][0, :, c], preferred_element_type=F32)
        sig = logistic(gate)
        silu = gate * sig
        act0[:, c] = (silu * up).astype(BF)
        p0[:, c] = up * (sig + silu * (1 - sig))
        s0[:, c] = silu
    ready(0, 2)
    h1[...] = (x[...].astype(F32) + jnp.dot(act0[...], bufs[2][0], preferred_element_type=F32).astype(BF).astype(F32)).astype(BF)
    normed(h1, a1_t)
    ready(1, 0, 1, 2)
    for f in range(BLOCKS):
        c = slice(f * width, (f + 1) * width)
        gate = jnp.dot(a_buf[...], bufs[0][1, :, c], preferred_element_type=F32)
        up = jnp.dot(a_buf[...], bufs[1][1, :, c], preferred_element_type=F32)
        d = lax.dot_general(dy[...], bufs[2][1, c, :], (((1,), (1,)), ((), ())), preferred_element_type=F32).astype(BF).astype(F32)
        sig = logistic(gate)
        silu = gate * sig
        act1[:, c] = (silu * up).astype(BF)
        dg1[:, c] = (d * up * (sig + silu * (1 - sig))).astype(BF)
        du1[:, c] = (d * silu).astype(BF)


def front(x, dy, weights):
    tokens, d = x.shape
    layers, _, ff = weights[0].shape
    count = tokens // FRONT_BLOCKS
    row = lambda n: pl.BlockSpec((count, n), lambda t: (t, 0))
    column = pl.BlockSpec((d, count), lambda t: (0, t))
    shape = jax.ShapeDtypeStruct
    return pl.pallas_call(
        front_kernel,
        grid=(FRONT_BLOCKS,),
        out_shape=[shape((tokens, ff), BF)] * 4 + [shape((tokens, ff), F32)] * 2 + [shape((tokens, d), BF)] + [shape((d, tokens), BF)] * 3,
        in_specs=[row(d)] * 2 + [ANY] * 3,
        out_specs=[row(ff)] * 6 + [row(d)] + [column] * 3,
        scratch_shapes=[pltpu.VMEM(w.shape, BF) for w in weights] + [pltpu.VMEM((count, d), BF), pltpu.SemaphoreType.DMA((layers, 3))],
        compiler_params=pltpu.CompilerParams(vmem_limit_bytes=VMEM_LIMIT, dimension_semantics=("arbitrary",)),
        name="front",
    )(x, dy, *weights)


def solution(mesh):
    n = mesh.shape["dp"]

    def step(x, dy, *arrays):
        weights, m, v = (arrays[i : i + 3] for i in (0, 3, 6))
        act0, act1, dg1, du1, p0, s0, h1, a0_t, a1_t, dy_t = front(x[0], dy[0], weights)
        return reduce_step_gather(n, dy_t, a1_t, a0_t, act1, dg1, du1, act0, p0, s0, h1, dy[0], weights, m, v)

    rows = P(None, "dp", None)
    return jax.shard_map(
        step,
        mesh=mesh,
        in_specs=(P(("rep", "dp"), None, None),) * 2 + (P(None, None, None),) * 3 + (rows,) * 6,
        out_specs=(P("rep", None, None),) * 3 + (P("rep", "dp", None),) * 6,
        check_vma=False,
    )
```
